32 devices in a mesh: dom: 8 (over z, y), sub: 4 (over x, core).
Axes of the slice: x: 2, y: 2, z: 4, core: 2. Of those that a mesh axis runs over, the one named last changes fastest.
Arguments:
- node_state: bfloat16 [64, 32768], P(None, ('dom', 'sub')), may hold values from -6 to 6
- edge_state: bfloat16 [64, 98304], P(None, ('dom', 'sub')), may hold values from -6 to 6
- senders: int32 [98304], P(('dom', 'sub')), may hold values from 0 to 2559, as said below
- receivers: int32 [98304], P(('dom', 'sub')), may hold values from 0 to 1023
- send_index: int32 [32, 12, 128], P(('dom', 'sub')), may hold values from -1 to 1023, as said below
- node_cotangent: bfloat16 [64, 32768], P(None, ('dom', 'sub')), may hold values from -6 to 6
- edge_cotangent: bfloat16 [64, 98304], P(None, ('dom', 'sub')), may hold values from -6 to 6
- edge_first: bfloat16 [192, 64], replicated, may hold values from -0.4375 to 0.4375
- edge_bias: float32 [64], replicated, may hold values from -3 to 3
- edge_second: bfloat16 [64, 64], replicated, may hold values from -0.75 to 0.75
- edge_gain: float32 [64], replicated, may hold values from 0.1 to 1.9
- edge_shift: float32 [64], replicated, may hold values from -3 to 3
- node_first: bfloat16 [128, 64], replicated, may hold values from -0.5 to 0.5
- node_bias: float32 [64], replicated, may hold values from -3 to 3
- node_second: bfloat16 [64, 64], replicated, may hold values from -0.75 to 0.75
- node_gain: float32 [64], replicated, may hold values from 0.1 to 1.9
Outputs:
- delta_state: bfloat16 [64, 32768], P(None, ('dom', 'sub'))
- delta_edges: bfloat16 [64, 98304], P(None, ('dom', 'sub'))
- delta_edgefirst: float32 [192, 64], replicated
- delta_edgebias: float32 [64], replicated
- delta_edgesecond: float32 [64, 64], replicated
- delta_edgegain: float32 [64], replicated
- delta_edgeshift: float32 [64], replicated
- delta_nodefirst: float32 [128, 64], replicated
- delta_nodebias: float32 [64], replicated
- delta_nodesecond: float32 [64, 64], replicated
- delta_nodegain: float32 [64], replicated
- delta_nodeshift: float32 [64], replicated
The draws below stay inside these ranges and needn't reach their ends.
Inputs may be any that keep to these rules, and one draw needn't show every extreme that they name: `send_index`: block k = o * 4 + t of partition p = d * 4 + s lists own cells that p sends to the partition at dom index d + o - 1 and sub index t: live entries first, then -1. Blocks towards a dom index outside the mesh, and block 4 + s, hold only -1; every other block holds 32 to 128 live entries. Some partition receives a full block from every partition that sends to it. `senders`: an entry below 1024 is an own cell. An entry 1024 + k * 128 + j with k = o * 4 + u names ghost slot j of block k: the j-th entry of block o * 4 + s of the partition at dom index d + 1 - o and sub index u, and that entry is live.
All inputs are finite; a program needn't handle non-finite values.
Results may differ from the reference program's by a relative error of at most 0.0095.
Values may be sent and summed in bfloat16 or wider, within the bound.
A program may use at most 64 MiB of HBM per device.

```python
import math
import jax
import jax.numpy as jnp
from jax import lax

D = 64
HIDDEN_SIZE = 64
CELLS_DEV = 1024
HALO = 128
FACES_DEV = 3072
PARTITIONS = 32
PEERS = 12
GHOST = 1536
CELLS = 32768
FACES = 98304
N_DOM = 8
N_SUB = 4


def halo_counts(key):
    base_key = jax.random.fold_in(key, 7)
    count_key, target_key = jax.random.split(base_key)
    live_count = jax.random.randint(count_key, (PARTITIONS, PEERS), HALO // 4, HALO + 1)
    partition = jnp.arange(PARTITIONS, dtype=jnp.int32)[:, None]
    peer_slot = jnp.arange(PEERS, dtype=jnp.int32)[None, :]
    target_row = partition // N_SUB + peer_slot // N_SUB - 1
    sub_here = partition % N_SUB
    exists = (target_row >= 0) & (target_row < N_DOM) & jnp.logical_not((peer_slot // N_SUB == 1) & (peer_slot % N_SUB == sub_here))
    chosen = jax.random.randint(target_key, (), N_SUB, PARTITIONS)
    target = target_row * N_SUB + peer_slot % N_SUB
    receives_full = target == chosen
    counts = jnp.where(receives_full, HALO, live_count)
    return jnp.where(exists, counts, 0).astype(jnp.int32)


def draw_send_index(key, part):
    counts = halo_counts(key)
    cell_draw = jax.random.randint(jax.random.fold_in(key, 11), (PARTITIONS, PEERS, HALO), 0, CELLS_DEV)
    slot_position = jnp.arange(HALO, dtype=jnp.int32)[None, None, :]
    return jnp.where(slot_position < counts[:, :, None], cell_draw, -1).astype(jnp.int32)


def draw_senders(key, part):
    counts = halo_counts(key)
    partition = jnp.arange(PARTITIONS, dtype=jnp.int32)[:, None]
    peer_slot = jnp.arange(PEERS, dtype=jnp.int32)[None, :]
    source_row = partition // N_SUB + 1 - peer_slot // N_SUB
    source_ok = (source_row >= 0) & (source_row < N_DOM)
    source = jnp.clip(source_row * N_SUB + peer_slot % N_SUB, 0, PARTITIONS - 1)
    mirror_slot = peer_slot // N_SUB * N_SUB + partition % N_SUB
    incoming = jnp.where(source_ok, counts[source, mirror_slot], 0)
    key_list = jax.random.split(jax.random.fold_in(key, 23), 4)
    local_cells = jax.random.randint(key_list[0], (PARTITIONS, FACES_DEV), 0, CELLS_DEV)
    chosen_peer = jax.random.randint(key_list[1], (PARTITIONS, FACES_DEV), 0, PEERS)
    position = jax.random.randint(key_list[2], (PARTITIONS, FACES_DEV), 0, HALO)
    want_ghost = jax.random.randint(key_list[3], (PARTITIONS, FACES_DEV), 0, 8) == 0
    face_number = jnp.arange(FACES_DEV, dtype=jnp.int32)[None, :]
    last_face = face_number == FACES_DEV - 1
    chosen_peer = jnp.where(last_face, PEERS - 1, chosen_peer)
    available = jnp.take_along_axis(incoming, chosen_peer, axis=1)
    position = jnp.where(last_face, available - 1, position % jnp.maximum(available, 1))
    use_ghost = (want_ghost | last_face) & (available > 0)
    ghost_index = CELLS_DEV + chosen_peer * HALO + position
    return jnp.where(use_ghost, ghost_index, local_cells).reshape(-1).astype(jnp.int32)


def place_ends(values, own_key, low, largest):
    shape = values.shape
    spot = [jax.random.randint(jax.random.fold_in(own_key, axis), (), 0, shape[axis]) for axis in range(len(shape))]
    values = values.at[tuple(spot)].set(low)
    longest = shape.index(max(shape))
    spot[longest] = (spot[longest] + 1) % shape[longest]
    return values.at[tuple(spot)].set(largest)


def level_of(key, extent, cuts, low, largest):
    level, own = 1.0, jax.random.fold_in(key, 6)
    for axis_at, shards_of in cuts:
        heights = jnp.exp(jax.random.uniform(jax.random.fold_in(own, axis_at), (shards_of,), jnp.float32, low / len(cuts), largest / len(cuts)))
        level = level * jnp.repeat(heights, extent[axis_at] // shards_of).reshape([-1 if axis == axis_at else 1 for axis in range(len(extent))])
    return level


def scatter_about(rng, shape, deviation, most, cuts=(), kind=jnp.bfloat16):
    factor_of = level_of(rng, shape, cuts, -0.22, 0.18) if cuts else 1.0
    values = jax.random.normal(rng, shape, jnp.float32) * deviation * factor_of
    return jnp.minimum(jnp.maximum(values, -most), most).astype(kind)


def setup_inputs(seed: int = 0) -> dict:
    splits = jax.random.split(jax.random.key(seed), 17)
    return {
        "node_state": scatter_about(splits[0], (D, CELLS), 1.0, 6.0, ((1, 32),)),
        "edge_state": scatter_about(splits[1], (D, FACES), 1.0, 6.0, ((1, 32),)),
        "senders": draw_senders(jax.random.fold_in(splits[16], 71), 0),
        "receivers": place_ends(jax.random.randint(splits[3], (FACES,), 0, CELLS_DEV), jax.random.fold_in(splits[3], 1), 0, CELLS_DEV - 1).astype(jnp.int32),
        "send_index": draw_send_index(jax.random.fold_in(splits[16], 71), 0),
        "node_cotangent": scatter_about(splits[5], (D, CELLS), 1.0, 6.0, ((1, 32),)),
        "edge_cotangent": scatter_about(splits[6], (D, FACES), 1.0, 6.0, ((1, 32),)),
        "edge_first": scatter_about(splits[7], (3 * D, HIDDEN_SIZE), (3 * D) ** -0.5, 0.4375),
        "edge_bias": scatter_about(splits[8], (HIDDEN_SIZE,), 0.5, 3.0, (), jnp.float32),
        "edge_second": scatter_about(splits[9], (HIDDEN_SIZE, D), HIDDEN_SIZE ** -0.5, 0.75),
        "edge_gain": jnp.clip(1.0 + 0.18 * jax.random.normal(splits[10], (D,), jnp.float32), 0.1, 1.9),
        "edge_shift": scatter_about(splits[11], (D,), 0.5, 3.0, (), jnp.float32),
        "node_first": scatter_about(splits[12], (2 * D, HIDDEN_SIZE), (2 * D) ** -0.5, 0.5),
        "node_bias": scatter_about(splits[13], (HIDDEN_SIZE,), 0.5, 3.0, (), jnp.float32),
        "node_second": scatter_about(splits[14], (HIDDEN_SIZE, D), HIDDEN_SIZE ** -0.5, 0.75),
        "node_gain": jnp.clip(1.0 + 0.18 * jax.random.normal(splits[15], (D,), jnp.float32), 0.1, 1.9),
    }


EPSILON = 1e-05

def contract_first(first_operand, second_operand):
    return lax.dot_general(first_operand, second_operand, (((0,), (0,)), ((), ())), preferred_element_type=jnp.float32)

def contract_last(first_operand, second_operand):
    return lax.dot_general(first_operand, second_operand, (((1,), (1,)), ((), ())), preferred_element_type=jnp.float32)

def sigmoid_linear(values):
    return values * jax.nn.sigmoid(values)

def sigmoid_slope(values):
    logistic = jax.nn.sigmoid(values)
    return logistic * (1.0 + values * (1.0 - logistic))

def standardize(values):
    centered = values - lax.optimization_barrier(jnp.mean(values, axis=0, keepdims=True))
    spread = lax.rsqrt(lax.optimization_barrier(jnp.mean(centered * centered, axis=0, keepdims=True)) + EPSILON)
    return (centered * spread, spread)

def normalize_back(upstream, scaled, spread, gain_vector):
    gain_delta = lax.optimization_barrier(jnp.sum(upstream * scaled, axis=1))
    shift_delta = lax.optimization_barrier(jnp.sum(upstream, axis=1))
    weighted = upstream * gain_vector[:, None]
    result = spread * (weighted - lax.optimization_barrier(jnp.mean(weighted, axis=0, keepdims=True)) - scaled * lax.optimization_barrier(jnp.mean(weighted * scaled, axis=0, keepdims=True)))
    return (result, gain_delta, shift_delta)

def local_backward(extended, node_state, edge_state, senders, receivers, node_cotangent, edge_cotangent, edge_first, edge_bias, edge_second, edge_gain, edge_shift, node_first, node_bias, node_second, node_gain):
    features, cell_count = node_state.shape
    sender_rows = jnp.take(extended, senders, axis=1)
    receiver_rows = jnp.take(node_state, receivers, axis=1)
    stacked = jnp.concatenate([sender_rows, receiver_rows, edge_state], axis=0)
    edge_linear = contract_first(edge_first, stacked) + edge_bias[:, None]
    edge_active = sigmoid_linear(edge_linear).astype(jnp.bfloat16)
    edge_output = contract_first(edge_second, edge_active)
    edge_scaled, edge_spread = standardize(edge_output)
    message = (edge_scaled * edge_gain[:, None] + edge_shift[:, None]).astype(jnp.bfloat16)
    summed = jnp.zeros((features, cell_count), jnp.float32).at[:, receivers].add(message.astype(jnp.float32))
    node_input = jnp.concatenate([node_state, summed.astype(jnp.bfloat16)], axis=0)
    node_linear = contract_first(node_first, node_input) + node_bias[:, None]
    node_active = sigmoid_linear(node_linear).astype(jnp.bfloat16)
    node_output = contract_first(node_second, node_active)
    node_scaled, node_spread = standardize(node_output)
    upstream = node_cotangent.astype(jnp.float32)
    node_delta, nodegain_delta, nodeshift_delta = normalize_back(upstream, node_scaled, node_spread, node_gain)
    node_delta = node_delta.astype(jnp.bfloat16)
    nodesecond_delta = contract_last(node_active, node_delta)
    node_hidden = jnp.dot(node_second, node_delta, preferred_element_type=jnp.float32) * sigmoid_slope(node_linear)
    nodebias_delta = lax.optimization_barrier(jnp.sum(node_hidden, axis=1))
    node_hidden = node_hidden.astype(jnp.bfloat16)
    nodefirst_delta = contract_last(node_input, node_hidden)
    node_back = jnp.dot(node_first, node_hidden, preferred_element_type=jnp.float32)
    message_delta = edge_cotangent.astype(jnp.float32) + jnp.take(node_back[features:], receivers, axis=1)
    edge_delta, edgegain_delta, edgeshift_delta = normalize_back(message_delta, edge_scaled, edge_spread, edge_gain)
    edge_delta = edge_delta.astype(jnp.bfloat16)
    edgesecond_delta = contract_last(edge_active, edge_delta)
    edge_hidden = jnp.dot(edge_second, edge_delta, preferred_element_type=jnp.float32) * sigmoid_slope(edge_linear)
    edgebias_delta = lax.optimization_barrier(jnp.sum(edge_hidden, axis=1))
    edge_hidden = edge_hidden.astype(jnp.bfloat16)
    edgefirst_delta = contract_last(stacked, edge_hidden)
    edge_back = jnp.dot(edge_first, edge_hidden, preferred_element_type=jnp.float32)
    edge_result = (edge_cotangent.astype(jnp.float32) + edge_back[2 * features:]).astype(jnp.bfloat16)
    scattered = jnp.zeros(extended.shape, jnp.float32).at[:, senders].add(edge_back[:features])
    local_delta = scattered[:, :cell_count].at[:, receivers].add(edge_back[features:2 * features]) + node_back[:features] + upstream
    ghost_delta = scattered[:, cell_count:]
    partials = (edgefirst_delta, edgebias_delta, edgesecond_delta, edgegain_delta, edgeshift_delta, nodefirst_delta, nodebias_delta, nodesecond_delta, nodegain_delta, nodeshift_delta)
    return (local_delta, ghost_delta, edge_result, partials)

def reference(node_state, edge_state, senders, receivers, send_index, node_cotangent, edge_cotangent, edge_first, edge_bias, edge_second, edge_gain, edge_shift, node_first, node_bias, node_second, node_gain):
    features = node_state.shape[0]
    partition = jnp.arange(PARTITIONS, dtype=jnp.int32)[:, None]
    peer_slot = jnp.arange(PEERS, dtype=jnp.int32)[None, :]
    slot_position = jnp.arange(HALO, dtype=jnp.int32)[None, None, :]
    mirror_slot = peer_slot // N_SUB * N_SUB + partition % N_SUB
    source_row = partition // N_SUB + 1 - peer_slot // N_SUB
    source_ok = (source_row >= 0) & (source_row < N_DOM)
    source = jnp.clip(source_row * N_SUB + peer_slot % N_SUB, 0, PARTITIONS - 1)
    incoming = send_index[source, mirror_slot]
    live_in = source_ok[:, :, None] & (incoming >= 0)
    global_in = source[:, :, None] * CELLS_DEV + jnp.maximum(incoming, 0)
    gathered = jnp.take(node_state, global_in.reshape(-1).astype(jnp.int32), axis=1)
    ghost_cells = jnp.where(live_in.reshape(1, -1), gathered, jnp.zeros_like(gathered))
    weight_shapes = (edge_first.shape, edge_bias.shape, edge_second.shape, edge_gain.shape, edge_gain.shape, node_first.shape, node_bias.shape, node_second.shape, node_gain.shape, node_gain.shape)
    initial = (jnp.zeros((features, CELLS), jnp.float32), jnp.zeros((features, PARTITIONS * GHOST), jnp.float32), jnp.zeros((features, FACES), jnp.bfloat16), tuple((jnp.zeros(shape, jnp.float32) for shape in weight_shapes)))

    def one_partition(loop_index, carried):
        local_all, ghost_all, edge_all, weight_all = carried
        cell_start = (loop_index * CELLS_DEV).astype(jnp.int32)
        face_start = (loop_index * FACES_DEV).astype(jnp.int32)
        ghost_start = (loop_index * GHOST).astype(jnp.int32)
        state_block = lax.dynamic_slice_in_dim(node_state, cell_start, CELLS_DEV, 1)
        ghost_block = lax.dynamic_slice_in_dim(ghost_cells, ghost_start, GHOST, 1)
        extended = jnp.concatenate([state_block, ghost_block], axis=1)
        outcome = local_backward(extended, state_block, lax.dynamic_slice_in_dim(edge_state, face_start, FACES_DEV, 1), lax.dynamic_slice_in_dim(senders, face_start, FACES_DEV, 0), lax.dynamic_slice_in_dim(receivers, face_start, FACES_DEV, 0), lax.dynamic_slice_in_dim(node_cotangent, cell_start, CELLS_DEV, 1), lax.dynamic_slice_in_dim(edge_cotangent, face_start, FACES_DEV, 1), edge_first, edge_bias, edge_second, edge_gain, edge_shift, node_first, node_bias, node_second, node_gain)
        local_delta, ghost_delta, edge_result, partials = outcome
        local_all = lax.dynamic_update_slice_in_dim(local_all, local_delta, cell_start, 1)
        ghost_all = lax.dynamic_update_slice_in_dim(ghost_all, ghost_delta, ghost_start, 1)
        edge_all = lax.dynamic_update_slice_in_dim(edge_all, edge_result, face_start, 1)
        weight_all = tuple((running + portion for running, portion in zip(weight_all, partials)))
        return (local_all, ghost_all, edge_all, weight_all)
    local_all, ghost_all, edge_all, weight_all = lax.fori_loop(0, PARTITIONS, one_partition, initial)
    target_row = partition // N_SUB + peer_slot // N_SUB - 1
    target_ok = (target_row >= 0) & (target_row < N_DOM)
    target = jnp.clip(target_row * N_SUB + peer_slot % N_SUB, 0, PARTITIONS - 1)
    live_out = target_ok[:, :, None] & (send_index >= 0)
    from_index = (target * PEERS + mirror_slot)[:, :, None] * HALO + slot_position
    coming_back = jnp.take(ghost_all, from_index.reshape(-1).astype(jnp.int32), axis=1)
    coming_back = jnp.where(live_out.reshape(1, -1), coming_back, jnp.zeros_like(coming_back))
    to_index = partition[:, :, None] * CELLS_DEV + jnp.maximum(send_index, 0)
    local_all = local_all.at[:, to_index.reshape(-1).astype(jnp.int32)].add(coming_back)
    factor = 1.0 / math.sqrt(FACES)
    edgefirst_sum, edgebias_sum, edgesecond_sum, edgegain_sum, edgeshift_sum, nodefirst_sum, nodebias_sum, nodesecond_sum, nodegain_sum, nodeshift_sum = weight_all
    return (local_all.astype(jnp.bfloat16), edge_all, edgefirst_sum * factor, edgebias_sum * factor, edgesecond_sum * factor, edgegain_sum * factor, edgeshift_sum * factor, nodefirst_sum * factor, nodebias_sum * factor, nodesecond_sum * factor, nodegain_sum * factor, nodeshift_sum * factor)
```

```python
import functools
import math

import jax
import jax.numpy as jnp
from jax import lax
from jax.experimental import pallas as pl
from jax.experimental.pallas import tpu as pltpu
from jax.sharding import PartitionSpec as P

EPSILON = 1e-05
MESH = pl.DeviceIdType.MESH
BF = jnp.bfloat16
F32 = jnp.float32


def nn(a, b):
    return lax.dot_general(a, b, (((1,), (0,)), ((), ())), preferred_element_type=F32)


def nt(a, b):
    return lax.dot_general(a, b, (((1,), (1,)), ((), ())), preferred_element_type=F32)


def flip(a):
    return a.astype(F32).T


def one_hot(index, rows):
    return jnp.where(lax.broadcasted_iota(jnp.int32, (rows, index.shape[1]), 0) == index, 1.0, 0.0).astype(BF)


def standardize(values):
    centered = values - jnp.mean(values, axis=0, keepdims=True)
    spread = lax.rsqrt(jnp.mean(centered * centered, axis=0, keepdims=True) + EPSILON)
    return centered * spread, spread


def normalize_back(upstream, scaled, spread, gain):
    weighted = upstream * gain
    return spread * (
        weighted
        - jnp.mean(weighted, axis=0, keepdims=True)
        - scaled * jnp.mean(weighted * scaled, axis=0, keepdims=True)
    )


def packed_rows(features):
    half = 3 * features // 2
    return half, half + features, half + 2 * features


def fold_lanes(values):
    total = values[:, :128]
    for begin in range(128, values.shape[1], 128):
        total = total + values[:, begin : begin + 128]
    return total


def halo_peers(dom, sub):
    d, s = lax.axis_index("dom"), lax.axis_index("sub")
    for o in (0, 2, 1):
        for r in range(sub):
            if o == 1 and r == 0:
                continue
            t = lax.rem(s + r, sub)
            target = d + (o - 1)
            yield o, t, target, (target >= 0) & (target < dom)


def halo_barrier_signal(dom, sub, barrier):
    for o, t, target, there in halo_peers(dom, sub):
        if o == 1:
            pl.semaphore_signal(barrier, inc=1, device_id=(target, t), device_id_type=MESH)
        else:
            @pl.when(there)
            def _():
                pl.semaphore_signal(barrier, inc=1, device_id=(target, t), device_id_type=MESH)


def halo_barrier_count(dom, sub):
    d = lax.axis_index("dom")
    ends = jnp.where(d > 0, sub, 0) + jnp.where(d < dom - 1, sub, 0)
    return ends + (sub - 1)


def pick_kernel(dom, sub, node_ref, index_ref, ghost_ref, outgoing, incoming, send_sem, recv_sem):
    d, s = lax.axis_index("dom"), lax.axis_index("sub")
    barrier = pltpu.get_barrier_semaphore()
    halo_barrier_signal(dom, sub, barrier)
    cells = node_ref.shape[1]
    halo = outgoing.shape[2]

    def pick(number, carry):
        chosen = index_ref[:, pl.ds(pl.multiple_of(number * 2 * halo, 2 * halo), 2 * halo)]
        picked = nn(node_ref[...], one_hot(chosen, cells)).astype(BF)
        outgoing[2 * number] = picked[:, :halo]
        outgoing[2 * number + 1] = picked[:, halo:]
        return carry

    lax.fori_loop(0, outgoing.shape[0] // 2, pick, 0)
    pl.semaphore_wait(barrier, halo_barrier_count(dom, sub))
    exchange(dom, sub, d, s, outgoing, incoming, send_sem, recv_sem, forward=True)
    for k in range(3 * sub):
        ghost_ref[:, k * halo : (k + 1) * halo] = incoming[k]


def halo_copy(outgoing, incoming, send_sem, recv_sem, source, landing, target, t):
    return pltpu.make_async_remote_copy(
        src_ref=outgoing.at[source],
        dst_ref=incoming.at[landing],
        send_sem=send_sem.at[source],
        recv_sem=recv_sem.at[landing],
        device_id=(target, t),
        device_id_type=MESH,
    )


def guarded(o, there, action):
    if o == 1:
        action()
    else:
        pl.when(there)(action)


def start_exchange(dom, sub, s, outgoing, incoming, send_sem, recv_sem, forward):
    for o, t, target, there in halo_peers(dom, sub):
        block = o if forward else 2 - o

        def start(block=block, t=t, target=target):
            halo_copy(outgoing, incoming, send_sem, recv_sem, block * sub + t, block * sub + s, target, t).start()

        guarded(o, there, start)
    d = lax.axis_index("dom")
    incoming[sub + s] = jnp.zeros(incoming.shape[1:], incoming.dtype)
    for o in (0, 2):
        origin = d + 1 - o if forward else d + o - 1

        @pl.when((origin < 0) | (origin >= dom))
        def _():
            for u in range(sub):
                incoming[o * sub + u] = jnp.zeros(incoming.shape[1:], incoming.dtype)


def finish_exchange(dom, sub, s, outgoing, incoming, send_sem, recv_sem, forward):
    for o, t, target, there in halo_peers(dom, sub):
        block = 2 - o if forward else o

        def finish(block=block, t=t, target=target):
            halo_copy(outgoing, incoming, send_sem, recv_sem, block * sub + t, block * sub + t, target, t).wait_recv()

        guarded(o, there, finish)
    for o, t, target, there in halo_peers(dom, sub):
        block = o if forward else 2 - o

        def finish(block=block, t=t, target=target):
            halo_copy(outgoing, incoming, send_sem, recv_sem, block * sub + t, block * sub + t, target, t).wait_send()

        guarded(o, there, finish)


def exchange(dom, sub, d, s, outgoing, incoming, send_sem, recv_sem, forward):
    start_exchange(dom, sub, s, outgoing, incoming, send_sem, recv_sem, forward)
    finish_exchange(dom, sub, s, outgoing, incoming, send_sem, recv_sem, forward)


def local_kernel(
    chunk,
    node_ref, ghost_ref, edge_ref, senders_ref, receivers_ref, node_cot_ref, edge_cot_ref,
    edge_first_ref, edge_second_ref, node_first_ref, node_second_ref, columns_ref,
    local_ref, ghost_delta_ref, edge_out_ref, packed_ref,
    selector, extended, slope, active, scaled_all, spread_all, summed, sums, small, lanes,
):
    features, cells = node_ref.shape
    faces = edge_ref.shape[1]
    ghosts = ghost_ref.shape[1]
    width = cells + ghosts
    step = 64
    extended[:, :cells] = node_ref[...]
    extended[:, cells:] = ghost_ref[...]
    edge_first_t = flip(edge_first_ref[...]).astype(BF)
    edge_second_t = flip(edge_second_ref[...]).astype(BF)
    edge_bias = columns_ref[:, 0:1]
    edge_gain = columns_ref[:, 1:2]
    edge_shift = columns_ref[:, 2:3]
    node_bias = columns_ref[:, 3:4]
    node_gain = columns_ref[:, 4:5]
    summed[...] = jnp.zeros(summed.shape, F32)
    row = lax.broadcasted_iota(jnp.int32, (step, chunk), 0)

    def forward(c, carry):
        here = pl.ds(pl.multiple_of(c * chunk, chunk), chunk)
        sender = senders_ref[:, here]
        receiver = receivers_ref[:, here]

        def fill(begin, index):
            def body(i, inner):
                at = pl.multiple_of(i * step, step)
                hit = row == (index - at)
                selector[c, pl.ds(pl.multiple_of(begin + at, step), step), :] = jnp.where(hit, 1.0, 0.0).astype(BF)
                return inner
            return body

        lax.fori_loop(0, width // step, fill(0, sender), 0)
        lax.fori_loop(0, cells // step, fill(width, receiver), 0)
        sent = nn(extended[...], selector[c, :width, :]).astype(BF)
        received = nn(node_ref[...], selector[c, width:, :]).astype(BF)
        stacked = jnp.concatenate([sent, received, edge_ref[:, here]], axis=0)
        linear = nn(edge_first_t, stacked) + edge_bias
        logistic = jax.nn.sigmoid(linear)
        lively = (linear * logistic).astype(BF)
        slope[:, here] = logistic * (1.0 + linear * (1.0 - logistic))
        active[:, here] = lively
        scaled, spread = standardize(nn(edge_second_t, lively))
        scaled_all[:, here] = scaled
        spread_all[:, here] = spread
        message = (scaled * edge_gain + edge_shift).astype(BF)
        summed[...] += nt(selector[c, width:, :], message)
        return carry

    lax.fori_loop(0, faces // chunk, forward, 0)

    node_first_t = flip(node_first_ref[...]).astype(BF)
    node_second_t = flip(node_second_ref[...]).astype(BF)
    node_input = jnp.concatenate([node_ref[...], summed[...].T.astype(BF)], axis=0)
    node_linear = nn(node_first_t, node_input) + node_bias
    node_logistic = jax.nn.sigmoid(node_linear)
    node_active = (node_linear * node_logistic).astype(BF)
    node_scaled, node_spread = standardize(nn(node_second_t, node_active))
    upstream = node_cot_ref[...].astype(F32)
    lanes[3] = fold_lanes(upstream * node_scaled)
    lanes[4] = fold_lanes(upstream)
    node_delta = normalize_back(upstream, node_scaled, node_spread, node_gain).astype(BF)
    node_slope = node_logistic * (1.0 + node_linear * (1.0 - node_logistic))
    node_hidden = nn(node_second_ref[...], node_delta) * node_slope
    lanes[5] = fold_lanes(node_hidden)
    node_hidden = node_hidden.astype(BF)
    node_first_delta = nt(node_input, node_hidden)
    half, mid, top = packed_rows(features)
    packed_ref[half:mid, :features] = node_first_delta[:features]
    packed_ref[half:mid, features:] = node_first_delta[features:]
    packed_ref[mid:top, features:] = nt(node_active, node_delta)
    node_back = nn(node_first_ref[...], node_hidden)
    local_ref[...] = node_back[:features] + upstream
    toward = node_back[features:]
    high = toward.astype(BF)
    low = (toward - high.astype(F32)).astype(BF)
    toward = jnp.concatenate([high, low], axis=0)

    sums[...] = jnp.zeros(sums.shape, F32)
    small[...] = jnp.zeros(small.shape, F32)
    for i in range(3):
        lanes[i] = jnp.zeros(lanes.shape[1:], F32)

    def backward(c, carry):
        here = pl.ds(pl.multiple_of(c * chunk, chunk), chunk)
        gathered = nn(toward, selector[c, width:, :])
        cotangent = edge_cot_ref[:, here].astype(F32)
        delta = cotangent + (gathered[:features] + gathered[features:])
        scaled = scaled_all[:, here]
        lanes[0] += fold_lanes(delta * scaled)
        lanes[1] += fold_lanes(delta)
        edge_delta = normalize_back(delta, scaled, spread_all[:, here], edge_gain).astype(BF)
        small[0] += nt(active[:, here], edge_delta)
        hidden = nn(edge_second_ref[...], edge_delta) * slope[:, here]
        lanes[2] += fold_lanes(hidden)
        hidden = hidden.astype(BF)
        edge_out_ref[:, here] = (cotangent + nn(edge_first_ref[2 * features :, :], hidden)).astype(BF)
        small[1] += nt(edge_ref[:, here], hidden)
        sums[...] += nt(selector[c], hidden)
        return carry

    lax.fori_loop(0, faces // chunk, backward, 0)

    by_sender = sums[:width, :].astype(BF)
    by_receiver = sums[width:, :].astype(BF)
    first = nn(extended[...], by_sender)
    second = nn(node_ref[...], by_receiver)
    packed_ref[0:features, :features] = first
    packed_ref[features:half, :features] = second[: half - features]
    packed_ref[0 : 2 * features - half, features:] = second[half - features :]
    packed_ref[2 * features - half : half, features:] = small[1]
    packed_ref[mid:top, :features] = small[0]
    column = lax.broadcasted_iota(jnp.int32, (features, 128), 1)
    vectors = jnp.zeros((features, 128), F32)
    for i in range(6):
        vectors = jnp.where(column == i, jnp.sum(lanes[i], axis=1, keepdims=True), vectors)
    packed_ref[top:, :] = jnp.zeros((packed_ref.shape[0] - top, 128), F32)
    packed_ref[top : top + 8, :features] = vectors.T[:8]
    back = nt(edge_first_ref[:features, :], by_sender)
    local_ref[...] += back[:, :cells] + nt(edge_first_ref[features : 2 * features, :], by_receiver)
    halo = ghost_delta_ref.shape[2]
    for k in range(ghosts // halo):
        ghost_delta_ref[k] = back[:, cells + k * halo : cells + (k + 1) * halo].astype(BF)


def finish_kernel(
    dom, sub, factor,
    ghost_ref, local_ref, index_ref, packed_ref,
    state_ref, edge_first_ref, edge_second_ref, node_first_ref, node_second_ref, vectors_ref,
    incoming, selector, scattered, pieces, reduced, gathered,
    send_sem, recv_sem, part_send, part_recv, whole_send, whole_recv,
):
    d, s = lax.axis_index("dom"), lax.axis_index("sub")
    count = dom * sub
    me = d * sub + s
    rows = reduced.shape[0]
    barrier = pltpu.get_barrier_semaphore()

    def place(r):
        other = lax.rem(me + r, count)
        return other, (other // sub, lax.rem(other, sub))

    def greet(r, carry):
        _, device = place(r)
        pl.semaphore_signal(barrier, inc=1, device_id=device, device_id_type=MESH)
        return carry

    lax.fori_loop(1, count, greet, 0)
    pl.semaphore_wait(barrier, count - 1)
    start_exchange(dom, sub, s, ghost_ref, incoming, send_sem, recv_sem, forward=False)

    def part_copy(source, landing, device):
        return pltpu.make_async_remote_copy(
            src_ref=packed_ref.at[pl.ds(pl.multiple_of(source * rows, 8), rows)],
            dst_ref=pieces.at[landing],
            send_sem=part_send.at[source],
            recv_sem=part_recv.at[landing],
            device_id=device,
            device_id_type=MESH,
        )

    def whole_copy(landing, device, other):
        return pltpu.make_async_remote_copy(
            src_ref=reduced,
            dst_ref=gathered.at[pl.ds(pl.multiple_of(landing * rows, 8), rows)],
            send_sem=whole_send.at[other],
            recv_sem=whole_recv.at[landing],
            device_id=device,
            device_id_type=MESH,
        )

    def send_part(r, carry):
        other, device = place(r)
        part_copy(other, me, device).start()
        return carry

    lax.fori_loop(1, count, send_part, 0)
    cells = state_ref.shape[1]
    span = selector.shape[2]

    def build(i, carry):
        selector[i] = one_hot(index_ref[:, pl.ds(pl.multiple_of(i * span, span), span)], cells)
        return carry

    lax.fori_loop(0, selector.shape[0], build, 0)
    own = pl.ds(pl.multiple_of(me * rows, 8), rows)

    def take_part(r, total):
        other, device = place(r)
        part_copy(other, other, device).wait_recv()
        return total + pieces[other]

    reduced[...] = lax.fori_loop(1, count, take_part, packed_ref[own, :])

    def send_whole(r, carry):
        other, device = place(r)
        whole_copy(me, device, other).start()
        return carry

    lax.fori_loop(1, count, send_whole, 0)
    gathered[own, :] = reduced[...]
    finish_exchange(dom, sub, s, ghost_ref, incoming, send_sem, recv_sem, forward=False)
    scattered[...] = jnp.zeros(scattered.shape, F32)

    def scatter(i, carry):
        value = jnp.concatenate([incoming[2 * i], incoming[2 * i + 1]], axis=1)
        scattered[...] += nt(selector[i], value)
        return carry

    lax.fori_loop(0, selector.shape[0], scatter, 0)
    state_ref[...] = (local_ref[...] + scattered[...].T).astype(BF)

    def settle(r, carry):
        other, device = place(r)
        whole_copy(other, device, other).wait_recv()
        return carry

    lax.fori_loop(1, count, settle, 0)

    def settle_sends(r, carry):
        other, device = place(r)
        part_copy(other, other, device).wait_send()
        whole_copy(other, device, other).wait_send()
        return carry

    lax.fori_loop(1, count, settle_sends, 0)
    features = node_second_ref.shape[0]
    half, mid, top = packed_rows(features)
    edge_first_ref[:half, :] = gathered[0:half, :features] * factor
    edge_first_ref[half:, :] = gathered[0:half, features:] * factor
    node_first_ref[:features, :] = gathered[half:mid, :features] * factor
    node_first_ref[features:, :] = gathered[half:mid, features:] * factor
    edge_second_ref[...] = gathered[mid:top, :features] * factor
    node_second_ref[...] = gathered[mid:top, features:] * factor
    vectors_ref[...] = gathered[top : top + 8, :features] * factor


def on_device(
    dom, sub,
    node_state, edge_state, senders, receivers, send_index, node_cotangent, edge_cotangent,
    edge_first, edge_bias, edge_second, edge_gain, edge_shift, node_first, node_bias, node_second, node_gain,
):
    features, cells = node_state.shape
    faces = edge_state.shape[1]
    halo = send_index.shape[2]
    peers = 3 * sub
    ghosts = peers * halo
    width = cells + ghosts
    count = dom * sub
    rows = -(-(packed_rows(features)[2] + 8) // (8 * count)) * 8
    chunk = math.gcd(faces, 512)
    vmem = pl.BlockSpec(memory_space=pltpu.VMEM)
    shape = jax.ShapeDtypeStruct
    dma = pltpu.SemaphoreType.DMA
    index_row = send_index.reshape(1, ghosts)
    ghost = pl.pallas_call(
        functools.partial(pick_kernel, dom, sub),
        out_shape=shape((features, ghosts), BF),
        in_specs=[vmem] * 2,
        out_specs=vmem,
        scratch_shapes=[
            pltpu.VMEM((peers, features, halo), BF),
            pltpu.VMEM((peers, features, halo), BF),
            dma((peers,)),
            dma((peers,)),
        ],
        compiler_params=pltpu.CompilerParams(collective_id=0, has_side_effects=True),
        name="halo_out",
    )(node_state, index_row)
    columns = jnp.stack([edge_bias, edge_gain, edge_shift, node_bias, node_gain], axis=1)
    local, ghost_delta, edge_result, packed = pl.pallas_call(
        functools.partial(local_kernel, chunk),
        out_shape=(
            shape((features, cells), F32),
            shape((peers, features, halo), BF),
            shape((features, faces), BF),
            shape((count * rows, 128), F32),
        ),
        in_specs=[vmem] * 12,
        out_specs=(vmem,) * 4,
        scratch_shapes=[
            pltpu.VMEM((faces // chunk, width + cells, chunk), BF),
            pltpu.VMEM((features, width), BF),
            pltpu.VMEM((features, faces), F32),
            pltpu.VMEM((features, faces), BF),
            pltpu.VMEM((features, faces), F32),
            pltpu.VMEM((1, faces), F32),
            pltpu.VMEM((cells, features), F32),
            pltpu.VMEM((width + cells, features), F32),
            pltpu.VMEM((2, features, features), F32),
            pltpu.VMEM((6, features, 128), F32),
        ],
        compiler_params=pltpu.CompilerParams(vmem_limit_bytes=60 * 1024 * 1024),
        name="local_layer",
    )(
        node_state, ghost, edge_state, senders.reshape(1, faces), receivers.reshape(1, faces),
        node_cotangent, edge_cotangent, edge_first, edge_second, node_first, node_second, columns,
    )
    state, edge_first_sum, edge_second_sum, node_first_sum, node_second_sum, vectors = pl.pallas_call(
        functools.partial(finish_kernel, dom, sub, 1.0 / math.sqrt(faces * count)),
        out_shape=(
            shape((features, cells), BF),
            shape(edge_first.shape, F32),
            shape(edge_second.shape, F32),
            shape(node_first.shape, F32),
            shape(node_second.shape, F32),
            shape((8, features), F32),
        ),
        in_specs=[vmem] * 4,
        out_specs=(vmem,) * 6,
        scratch_shapes=[
            pltpu.VMEM((peers, features, halo), BF),
            pltpu.VMEM((peers // 2, cells, 2 * halo), BF),
            pltpu.VMEM((cells, features), F32),
            pltpu.VMEM((count, rows, 128), F32),
            pltpu.VMEM((rows, 128), F32),
            pltpu.VMEM((count * rows, 128), F32),
            dma((peers,)),
            dma((peers,)),
            dma((count,)),
            dma((count,)),
            dma((count,)),
            dma((count,)),
        ],
        compiler_params=pltpu.CompilerParams(collective_id=1, has_side_effects=True),
        name="halo_back_and_sum",
    )(ghost_delta, local, index_row, packed)
    return (
        state, edge_result, edge_first_sum, vectors[2], edge_second_sum, vectors[0], vectors[1],
        node_first_sum, vectors[5], node_second_sum, vectors[3], vectors[4],
    )


def solution(mesh):
    split = P(None, ("dom", "sub"))
    faces = P(("dom", "sub"))
    return jax.shard_map(
        functools.partial(on_device, mesh.shape["dom"], mesh.shape["sub"]),
        mesh=mesh,
        in_specs=(split, split, faces, faces, P(("dom", "sub"), None, None), split, split) + (P(),) * 9,
        out_specs=(split, split) + (P(),) * 10,
        check_vma=False,
    )
```

```python
import functools
import math

import jax
import jax.numpy as jnp
from jax import lax
from jax.experimental import pallas as pl
from jax.experimental.pallas import tpu as pltpu
from jax.sharding import PartitionSpec as P

EPSILON = 1e-05
MESH = pl.DeviceIdType.MESH
BF = jnp.bfloat16
F32 = jnp.float32


def nn(a, b):
    return lax.dot_general(a, b, (((1,), (0,)), ((), ())), preferred_element_type=F32)


def nt(a, b):
    return lax.dot_general(a, b, (((1,), (1,)), ((), ())), preferred_element_type=F32)


def flip(a):
    return a.astype(F32).T


def one_hot(index, rows):
    return jnp.where(lax.broadcasted_iota(jnp.int32, (rows, index.shape[1]), 0) == index, 1.0, 0.0).astype(BF)


def standardize(values):
    centered = values - jnp.mean(values, axis=0, keepdims=True)
    spread = lax.rsqrt(jnp.mean(centered * centered, axis=0, keepdims=True) + EPSILON)
    return centered * spread, spread


def normalize_back(upstream, scaled, spread, gain):
    weighted = upstream * gain
    return spread * (
        weighted
        - jnp.mean(weighted, axis=0, keepdims=True)
        - scaled * jnp.mean(weighted * scaled, axis=0, keepdims=True)
    )


def packed_rows(features):
    half = 3 * features // 2
    return half, half + features, half + 2 * features


def fold_lanes(values):
    total = values[:, :128]
    for begin in range(128, values.shape[1], 128):
        total = total + values[:, begin : begin + 128]
    return total


def halo_peers(dom, sub):
    d, s = lax.axis_index("dom"), lax.axis_index("sub")
    for o in (0, 2, 1):
        for r in range(sub):
            if o == 1 and r == 0:
                continue
            t = lax.rem(s + r, sub)
            target = d + (o - 1)
            yield o, t, target, (target >= 0) & (target < dom)


def halo_copy(outgoing, incoming, send_sem, recv_sem, source, landing, target, t):
    return pltpu.make_async_remote_copy(
        src_ref=outgoing.at[source],
        dst_ref=incoming.at[landing],
        send_sem=send_sem.at[source],
        recv_sem=recv_sem.at[landing],
        device_id=(target, t),
        device_id_type=MESH,
    )


def guarded(o, there, action):
    if o == 1:
        action()
    else:
        pl.when(there)(action)


def start_exchange(dom, sub, s, outgoing, incoming, send_sem, recv_sem, forward):
    for o, t, target, there in halo_peers(dom, sub):
        block = o if forward else 2 - o

        def start(block=block, t=t, target=target):
            halo_copy(outgoing, incoming, send_sem, recv_sem, block * sub + t, block * sub + s, target, t).start()

        guarded(o, there, start)
    d = lax.axis_index("dom")
    incoming[sub + s] = jnp.zeros(incoming.shape[1:], incoming.dtype)
    for o in (0, 2):
        origin = d + 1 - o if forward else d + o - 1

        @pl.when((origin < 0) | (origin >= dom))
        def _():
            for u in range(sub):
                incoming[o * sub + u] = jnp.zeros(incoming.shape[1:], incoming.dtype)


def finish_exchange(dom, sub, s, outgoing, incoming, send_sem, recv_sem, forward):
    for o, t, target, there in halo_peers(dom, sub):
        block = 2 - o if forward else o

        def finish(block=block, t=t, target=target):
            halo_copy(outgoing, incoming, send_sem, recv_sem, block * sub + t, block * sub + t, target, t).wait_recv()

        guarded(o, there, finish)
    for o, t, target, there in halo_peers(dom, sub):
        block = o if forward else 2 - o

        def finish(block=block, t=t, target=target):
            halo_copy(outgoing, incoming, send_sem, recv_sem, block * sub + t, block * sub + t, target, t).wait_send()

        guarded(o, there, finish)


def layer_kernel(
    dom, sub, chunk,
    node_ref, edge_ref, senders_ref, receivers_ref, index_ref, node_cot_ref, edge_cot_ref,
    edge_first_ref, edge_second_ref, node_first_ref, node_second_ref,
    edge_bias_ref, edge_gain_ref, edge_shift_ref, node_bias_ref, node_gain_ref,
    state_ref, edge_out_ref, sum_ref,
    outgoing, incoming, returning, returned, exports,
    selector, extended, slope, active, scaled_all, spread_all, summed, sums, small, lanes, local,
    packed_ref, pieces, reduced,
    send_sem, recv_sem, back_send, back_recv, part_send, part_recv, whole_send, whole_recv,
):
    features, cells = node_ref.shape
    faces = edge_ref.shape[1]
    peers, _, halo = outgoing.shape
    width = extended.shape[1]
    step = 128
    d, s = lax.axis_index("dom"), lax.axis_index("sub")
    count = dom * sub
    me = d * sub + s
    rows = reduced.shape[0]
    barrier = pltpu.get_barrier_semaphore()

    def place(r):
        other = lax.rem(me + r, count)
        return other, (other // sub, lax.rem(other, sub))

    def greet(r, carry):
        _, device = place(r)
        pl.semaphore_signal(barrier, inc=1, device_id=device, device_id_type=MESH)
        return carry

    lax.fori_loop(1, count, greet, 0)

    def pick(number, carry):
        chosen = index_ref[:, pl.ds(pl.multiple_of(number * 2 * halo, 2 * halo), 2 * halo)]
        exports[number] = one_hot(chosen, cells)
        picked = nn(node_ref[...], exports[number]).astype(BF)
        outgoing[2 * number] = picked[:, :halo]
        outgoing[2 * number + 1] = picked[:, halo:]
        return carry

    lax.fori_loop(0, peers // 2, pick, 0)
    pl.semaphore_wait(barrier, count - 1)
    start_exchange(dom, sub, s, outgoing, incoming, send_sem, recv_sem, forward=True)

    edge_first_t = edge_first_ref[...]
    edge_first = flip(edge_first_t).astype(BF)
    edge_second = edge_second_ref[...]
    edge_second_t = flip(edge_second).astype(BF)
    vectors = [edge_bias_ref, edge_gain_ref, edge_shift_ref, node_bias_ref, node_gain_ref]
    table = jnp.concatenate([v[...] for v in vectors] + [jnp.zeros((3, features), F32)], axis=0).T
    edge_bias, edge_gain, edge_shift, node_bias, node_gain = (table[:, i : i + 1] for i in range(5))
    summed[...] = jnp.zeros(summed.shape, F32)
    row = lax.broadcasted_iota(jnp.int32, (step, chunk), 0)

    def prepare(c, carry):
        here = pl.ds(pl.multiple_of(c * chunk, chunk), chunk)
        sender = senders_ref[:, here]
        receiver = receivers_ref[:, here]

        def fill(begin, index):
            def body(i, inner):
                at = pl.multiple_of(i * step, step)
                hit = row == (index - at)
                selector[c, pl.ds(pl.multiple_of(begin + at, step), step), :] = jnp.where(hit, 1.0, 0.0).astype(BF)
                return inner
            return body

        lax.fori_loop(0, width // step, fill(0, sender), 0)
        lax.fori_loop(0, cells // step, fill(width, receiver), 0)
        received = nn(node_ref[...], selector[c, width:, :]).astype(BF)
        stacked = jnp.concatenate([received, edge_ref[:, here]], axis=0)
        slope[:, here] = nn(edge_first_t[:, features:], stacked) + edge_bias
        return carry

    lax.fori_loop(0, faces // chunk, prepare, 0)
    finish_exchange(dom, sub, s, outgoing, incoming, send_sem, recv_sem, forward=True)
    extended[:, :cells] = node_ref[...]
    for k in range(peers):
        extended[:, cells + k * halo : cells + (k + 1) * halo] = incoming[k]

    def forward(c, carry):
        here = pl.ds(pl.multiple_of(c * chunk, chunk), chunk)
        sent = nn(extended[...], selector[c, :width, :]).astype(BF)
        linear = nn(edge_first_t[:, :features], sent) + slope[:, here]
        logistic = jax.nn.sigmoid(linear)
        lively = (linear * logistic).astype(BF)
        slope[:, here] = logistic * (1.0 + linear * (1.0 - logistic))
        active[:, here] = lively
        scaled, spread = standardize(nn(edge_second_t, lively))
        scaled_all[:, here] = scaled
        spread_all[:, here] = spread
        message = (scaled * edge_gain + edge_shift).astype(BF)
        summed[...] += nt(selector[c, width:, :], message)
        return carry

    lax.fori_loop(0, faces // chunk, forward, 0)

    node_first_t = node_first_ref[...]
    node_first = flip(node_first_t).astype(BF)
    node_second_t = flip(node_second_ref[...]).astype(BF)
    node_input = jnp.concatenate([node_ref[...], summed[...].T.astype(BF)], axis=0)
    node_linear = nn(node_first_t, node_input) + node_bias
    node_logistic = jax.nn.sigmoid(node_linear)
    node_active = (node_linear * node_logistic).astype(BF)
    node_scaled, node_spread = standardize(nn(node_second_t, node_active))
    upstream = node_cot_ref[...].astype(F32)
    lanes[3] = fold_lanes(upstream * node_scaled)
    lanes[4] = fold_lanes(upstream)
    node_delta = normalize_back(upstream, node_scaled, node_spread, node_gain).astype(BF)
    node_slope = node_logistic * (1.0 + node_linear * (1.0 - node_logistic))
    node_hidden = nn(node_second_ref[...], node_delta) * node_slope
    lanes[5] = fold_lanes(node_hidden)
    node_hidden = node_hidden.astype(BF)
    node_first_delta = nt(node_input, node_hidden)
    half, mid, top = packed_rows(features)
    packed_ref[half:mid, :features] = node_first_delta[:features]
    packed_ref[half:mid, features:] = node_first_delta[features:]
    packed_ref[mid:top, features:] = nt(node_active, node_delta)
    node_back = nn(node_first, node_hidden)
    local[...] = node_back[:features] + upstream
    toward = node_back[features:]
    high = toward.astype(BF)
    low = (toward - high.astype(F32)).astype(BF)
    toward = jnp.concatenate([high, low], axis=0)

    sums[...] = jnp.zeros(sums.shape, F32)
    small[...] = jnp.zeros(small.shape, F32)
    for i in range(3):
        lanes[i] = jnp.zeros(lanes.shape[1:], F32)

    def backward(c, carry):
        here = pl.ds(pl.multiple_of(c * chunk, chunk), chunk)
        gathered = nn(toward, selector[c, width:, :])
        cotangent = edge_cot_ref[:, here].astype(F32)
        delta = cotangent + (gathered[:features] + gathered[features:])
        scaled = scaled_all[:, here]
        lanes[0] += fold_lanes(delta * scaled)
        lanes[1] += fold_lanes(delta)
        edge_delta = normalize_back(delta, scaled, spread_all[:, here], edge_gain).astype(BF)
        small[0] += nt(active[:, here], edge_delta)
        hidden = nn(edge_second, edge_delta) * slope[:, here]
        lanes[2] += fold_lanes(hidden)
        hidden = hidden.astype(BF)
        active[:, here] = hidden
        small[1] += nt(edge_ref[:, here], hidden)
        sums[...] += nt(selector[c], hidden)
        return carry

    lax.fori_loop(0, faces // chunk, backward, 0)

    by_sender = sums[:width, :].astype(BF)
    by_receiver = sums[width:, :].astype(BF)
    back = nt(edge_first[:features], by_sender)
    for k in range(peers):
        returning[k] = back[:, cells + k * halo : cells + (k + 1) * halo].astype(BF)
    first = nn(extended[...], by_sender)
    second = nn(node_ref[...], by_receiver)
    packed_ref[0:features, :features] = first
    packed_ref[features:half, :features] = second[: half - features]
    packed_ref[0 : 2 * features - half, features:] = second[half - features :]
    packed_ref[2 * features - half : half, features:] = small[1]
    packed_ref[mid:top, :features] = small[0]
    column = lax.broadcasted_iota(jnp.int32, (features, 128), 1)
    vectors = jnp.zeros((features, 128), F32)
    for i in range(6):
        vectors = jnp.where(column == i, jnp.sum(lanes[i], axis=1, keepdims=True), vectors)
    packed_ref[top:, :] = jnp.zeros((packed_ref.shape[0] - top, 128), F32)
    packed_ref[top : top + 8, :features] = vectors.T[:8]

    def part_copy(source, landing, device):
        return pltpu.make_async_remote_copy(
            src_ref=packed_ref.at[pl.ds(pl.multiple_of(source * rows, 8), rows)],
            dst_ref=pieces.at[landing],
            send_sem=part_send.at[source],
            recv_sem=part_recv.at[landing],
            device_id=device,
            device_id_type=MESH,
        )

    def whole_copy(landing, device, other):
        return pltpu.make_async_remote_copy(
            src_ref=reduced,
            dst_ref=sum_ref.at[pl.ds(pl.multiple_of(landing * rows, 8), rows)],
            send_sem=whole_send.at[other],
            recv_sem=whole_recv.at[landing],
            device_id=device,
            device_id_type=MESH,
        )

    def send_part(r, carry):
        other, device = place(r)
        part_copy(other, me, device).start()
        return carry

    lax.fori_loop(1, count, send_part, 0)
    start_exchange(dom, sub, s, returning, returned, back_send, back_recv, forward=False)
    local[...] += back[:, :cells] + nt(edge_first[features : 2 * features], by_receiver)

    def emit(c, carry):
        here = pl.ds(pl.multiple_of(c * chunk, chunk), chunk)
        ahead = nn(edge_first[2 * features :], active[:, here])
        edge_out_ref[:, here] = (edge_cot_ref[:, here].astype(F32) + ahead).astype(BF)
        return carry

    lax.fori_loop(0, faces // chunk, emit, 0)
    own = pl.ds(pl.multiple_of(me * rows, 8), rows)

    def take_part(r, total):
        other, device = place(r)
        part_copy(other, other, device).wait_recv()
        return total + pieces[other]

    reduced[...] = lax.fori_loop(1, count, take_part, packed_ref[own, :])

    def send_whole(r, carry):
        other, device = place(r)
        whole_copy(me, device, other).start()
        return carry

    lax.fori_loop(1, count, send_whole, 0)
    sum_ref[own, :] = reduced[...]
    finish_exchange(dom, sub, s, returning, returned, back_send, back_recv, forward=False)
    summed[...] = jnp.zeros(summed.shape, F32)

    def scatter(i, carry):
        value = jnp.concatenate([returned[2 * i], returned[2 * i + 1]], axis=1)
        summed[...] += nt(exports[i], value)
        return carry

    lax.fori_loop(0, peers // 2, scatter, 0)
    state_ref[...] = (local[...] + summed[...].T).astype(BF)

    def settle(r, carry):
        other, device = place(r)
        part_copy(other, other, device).wait_send()
        whole_copy(other, device, other).wait_send()
        whole_copy(other, device, other).wait_recv()
        return carry

    lax.fori_loop(1, count, settle, 0)


def unpack_kernel(
    factor, state_in, edge_in, sum_ref,
    state_ref, edge_ref, edge_first_ref, edge_second_ref, node_first_ref, node_second_ref, *vector_refs,
):
    features = state_in.shape[0]
    half, mid, top = packed_rows(features)
    state_ref[...] = state_in[...]
    edge_ref[...] = edge_in[...]
    left = sum_ref[:, :features] * factor
    right = sum_ref[:, features:] * factor
    edge_first_ref[...] = jnp.concatenate([left[:half], right[:half]], axis=0).T
    node_first_ref[...] = jnp.concatenate([left[half:mid], right[half:mid]], axis=0).T
    edge_second_ref[...] = left[mid:top]
    node_second_ref[...] = right[mid:top]
    for i, vector_ref in enumerate(vector_refs):
        vector_ref[...] = left[top + i : top + i + 1]


def on_device(
    dom, sub,
    node_state, edge_state, senders, receivers, send_index, node_cotangent, edge_cotangent,
    edge_first, edge_bias, edge_second, edge_gain, edge_shift, node_first, node_bias, node_second, node_gain,
):
    features, cells = node_state.shape
    faces = edge_state.shape[1]
    halo = send_index.shape[2]
    peers = 3 * sub
    ghosts = peers * halo
    width = cells + ghosts
    count = dom * sub
    rows = -(-(packed_rows(features)[2] + 8) // (8 * count)) * 8
    chunk = math.gcd(faces, 512)
    vmem = pl.BlockSpec(memory_space=pltpu.VMEM)
    shape = jax.ShapeDtypeStruct
    dma = pltpu.SemaphoreType.DMA

    def line(vector):
        return vector.reshape(1, -1)

    state, edge_result, total = pl.pallas_call(
        functools.partial(layer_kernel, dom, sub, chunk),
        out_shape=(
            shape((features, cells), BF),
            shape((features, faces), BF),
            shape((count * rows, 128), F32),
        ),
        in_specs=[vmem] * 16,
        out_specs=(vmem,) * 3,
        scratch_shapes=[pltpu.VMEM((peers, features, halo), BF)] * 4
        + [
            pltpu.VMEM((peers // 2, cells, 2 * halo), BF),
            pltpu.VMEM((faces // chunk, width + cells, chunk), BF),
            pltpu.VMEM((features, width), BF),
            pltpu.VMEM((features, faces), F32),
            pltpu.VMEM((features, faces), BF),
            pltpu.VMEM((features, faces), F32),
            pltpu.VMEM((1, faces), F32),
            pltpu.VMEM((cells, features), F32),
            pltpu.VMEM((width + cells, features), F32),
            pltpu.VMEM((2, features, features), F32),
            pltpu.VMEM((6, features, 128), F32),
            pltpu.VMEM((features, cells), F32),
            pltpu.VMEM((count * rows, 128), F32),
            pltpu.VMEM((count, rows, 128), F32),
            pltpu.VMEM((rows, 128), F32),
        ]
        + [dma((peers,))] * 4
        + [dma((count,))] * 4,
        compiler_params=pltpu.CompilerParams(
            collective_id=0, has_side_effects=True, vmem_limit_bytes=60 * 1024 * 1024
        ),
        name="layer",
    )(
        node_state, edge_state, line(senders), line(receivers), line(send_index),
        node_cotangent, edge_cotangent, edge_first.T, edge_second, node_first.T, node_second,
        line(edge_bias), line(edge_gain), line(edge_shift), line(node_bias), line(node_gain),
    )
    vector = shape((1, features), F32)
    state, edge_result, edge_first_sum, edge_second_sum, node_first_sum, node_second_sum, *vectors = pl.pallas_call(
        functools.partial(unpack_kernel, 1.0 / math.sqrt(faces * count)),
        out_shape=(
            shape((features, cells), BF),
            shape((features, faces), BF),
            shape(edge_first.shape[::-1], F32),
            shape(edge_second.shape, F32),
            shape(node_first.shape[::-1], F32),
            shape(node_second.shape, F32),
        )
        + (vector,) * 6,
        in_specs=[vmem] * 3,
        out_specs=(vmem,) * 12,
        name="unpack",
    )(state, edge_result, total)
    vectors = [v.reshape(-1) for v in vectors]
    return (
        state, edge_result, edge_first_sum.T, vectors[2], edge_second_sum, vectors[0], vectors[1],
        node_first_sum.T, vectors[5], node_second_sum, vectors[3], vectors[4],
    )


def solution(mesh):
    split = P(None, ("dom", "sub"))
    faces = P(("dom", "sub"))
    return jax.shard_map(
        functools.partial(on_device, mesh.shape["dom"], mesh.shape["sub"]),
        mesh=mesh,
        in_specs=(split, split, faces, faces, P(("dom", "sub"), None, None), split, split) + (P(),) * 9,
        out_specs=(split, split) + (P(),) * 10,
        check_vma=False,
    )
```

```python
import functools
import math

import jax
import jax.numpy as jnp
from jax import lax
from jax.experimental import pallas as pl
from jax.experimental.pallas import tpu as pltpu
from jax.sharding import PartitionSpec as P

EPSILON = 1e-05
MESH = pl.DeviceIdType.MESH
BF = jnp.bfloat16
F32 = jnp.float32


def nn(a, b):
    return lax.dot_general(a, b, (((1,), (0,)), ((), ())), preferred_element_type=F32)


def nt(a, b):
    return lax.dot_general(a, b, (((1,), (1,)), ((), ())), preferred_element_type=F32)


def flip(a):
    return a.astype(F32).T


def one_hot(index, rows):
    return jnp.where(lax.broadcasted_iota(jnp.int32, (rows, index.shape[1]), 0) == index, 1.0, 0.0).astype(BF)


def standardize(values):
    centered = values - jnp.mean(values, axis=0, keepdims=True)
    spread = lax.rsqrt(jnp.mean(centered * centered, axis=0, keepdims=True) + EPSILON)
    return centered * spread, spread


def normalize_back(upstream, scaled, spread, gain):
    weighted = upstream * gain
    return spread * (
        weighted
        - jnp.mean(weighted, axis=0, keepdims=True)
        - scaled * jnp.mean(weighted * scaled, axis=0, keepdims=True)
    )


def packed_rows(features):
    half = 3 * features // 2
    return half, half + features, half + 2 * features


def fold_lanes(values):
    total = values[:, :128]
    for begin in range(128, values.shape[1], 128):
        total = total + values[:, begin : begin + 128]
    return total


def halo_peers(dom, sub):
    d, s = lax.axis_index("dom"), lax.axis_index("sub")
    for o in (0, 2, 1):
        for r in range(sub):
            if o == 1 and r == 0:
                continue
            t = lax.rem(s + r, sub)
            target = d + (o - 1)
            yield o, t, target, (target >= 0) & (target < dom)


def halo_copy(outgoing, incoming, send_sem, recv_sem, source, landing, target, t):
    return pltpu.make_async_remote_copy(
        src_ref=outgoing.at[source],
        dst_ref=incoming.at[landing],
        send_sem=send_sem.at[source],
        recv_sem=recv_sem.at[landing],
        device_id=(target, t),
        device_id_type=MESH,
    )


def guarded(o, there, action):
    if o == 1:
        action()
    else:
        pl.when(there)(action)


def start_exchange(dom, sub, s, outgoing, incoming, send_sem, recv_sem, forward):
    for o, t, target, there in halo_peers(dom, sub):
        block = o if forward else 2 - o

        def start(block=block, t=t, target=target):
            halo_copy(outgoing, incoming, send_sem, recv_sem, block * sub + t, block * sub + s, target, t).start()

        guarded(o, there, start)
    d = lax.axis_index("dom")
    incoming[sub + s] = jnp.zeros(incoming.shape[1:], incoming.dtype)
    for o in (0, 2):
        origin = d + 1 - o if forward else d + o - 1

        @pl.when((origin < 0) | (origin >= dom))
        def _():
            for u in range(sub):
                incoming[o * sub + u] = jnp.zeros(incoming.shape[1:], incoming.dtype)


def finish_exchange(dom, sub, s, outgoing, incoming, send_sem, recv_sem, forward):
    for o, t, target, there in halo_peers(dom, sub):
        block = 2 - o if forward else o

        def finish(block=block, t=t, target=target):
            halo_copy(outgoing, incoming, send_sem, recv_sem, block * sub + t, block * sub + t, target, t).wait_recv()

        guarded(o, there, finish)
    for o, t, target, there in halo_peers(dom, sub):
        block = o if forward else 2 - o

        def finish(block=block, t=t, target=target):
            halo_copy(outgoing, incoming, send_sem, recv_sem, block * sub + t, block * sub + t, target, t).wait_send()

        guarded(o, there, finish)


def layer_kernel(
    dom, sub, chunk,
    node_ref, edge_ref, senders_ref, receivers_ref, index_ref, node_cot_ref, edge_cot_ref,
    edge_first_ref, edge_second_ref, node_first_ref, node_second_ref,
    edge_bias_ref, edge_gain_ref, edge_shift_ref, node_bias_ref, node_gain_ref,
    state_ref, edge_out_ref, sum_ref,
    outgoing, incoming, returning, returned, exports,
    selector, extended, slope, active, scaled_all, spread_all, summed, sums, small, lanes, local,
    packed_ref, pieces, reduced,
    send_sem, recv_sem, back_send, back_recv, part_send, part_recv, whole_send, whole_recv,
):
    features, cells = node_ref.shape
    faces = edge_ref.shape[1]
    peers, _, halo = outgoing.shape
    width = extended.shape[1]
    step = 128
    d, s = lax.axis_index("dom"), lax.axis_index("sub")
    count = dom * sub
    me = d * sub + s
    rows = reduced.shape[0]
    barrier = pltpu.get_barrier_semaphore()

    def place(r):
        other = lax.rem(me + r, count)
        return other, (other // sub, lax.rem(other, sub))

    def greet(r, carry):
        _, device = place(r)
        pl.semaphore_signal(barrier, inc=1, device_id=device, device_id_type=MESH)
        return carry

    lax.fori_loop(1, count, greet, 0)

    def pick(number, carry):
        chosen = index_ref[:, pl.ds(pl.multiple_of(number * 2 * halo, 2 * halo), 2 * halo)]
        exports[number] = one_hot(chosen, cells)
        picked = nn(node_ref[...], exports[number]).astype(BF)
        outgoing[2 * number] = picked[:, :halo]
        outgoing[2 * number + 1] = picked[:, halo:]
        return carry

    lax.fori_loop(0, peers // 2, pick, 0)
    pl.semaphore_wait(barrier, count - 1)
    start_exchange(dom, sub, s, outgoing, incoming, send_sem, recv_sem, forward=True)

    edge_first_t = edge_first_ref[...]
    edge_first = flip(edge_first_t).astype(BF)
    edge_second = edge_second_ref[...]
    edge_second_t = flip(edge_second).astype(BF)
    vectors = [edge_bias_ref, edge_gain_ref, edge_shift_ref, node_bias_ref, node_gain_ref]
    table = jnp.concatenate([v[...] for v in vectors] + [jnp.zeros((3, features), F32)], axis=0).T
    edge_bias, edge_gain, edge_shift, node_bias, node_gain = (table[:, i : i + 1] for i in range(5))
    summed[...] = jnp.zeros(summed.shape, F32)
    row = lax.broadcasted_iota(jnp.int32, (step, chunk), 0)
    one, zero = jnp.ones((step, chunk), BF), jnp.zeros((step, chunk), BF)

    def prepare(c, carry):
        here = pl.ds(pl.multiple_of(c * chunk, chunk), chunk)
        sender = senders_ref[:, here]
        receiver = receivers_ref[:, here]

        def fill(begin, index):
            offset = (jnp.broadcast_to(index, (step, chunk)) - row).astype(jnp.int16)

            def body(i, inner):
                at = pl.multiple_of(i * step, step)
                hit = offset == jnp.full((step, chunk), at, jnp.int32).astype(jnp.int16)
                selector[c, pl.ds(pl.multiple_of(begin + at, step), step), :] = jnp.where(hit, one, zero)
                return inner
            return body

        lax.fori_loop(0, width // step, fill(0, sender), 0)
        lax.fori_loop(0, cells // step, fill(width, receiver), 0)
        received = nn(node_ref[...], selector[c, width:, :]).astype(BF)
        stacked = jnp.concatenate([received, edge_ref[:, here]], axis=0)
        slope[:, here] = nn(edge_first_t[:, features:], stacked) + edge_bias
        return carry

    lax.fori_loop(0, faces // chunk, prepare, 0)
    finish_exchange(dom, sub, s, outgoing, incoming, send_sem, recv_sem, forward=True)
    extended[:, :cells] = node_ref[...]
    for k in range(peers):
        extended[:, cells + k * halo : cells + (k + 1) * halo] = incoming[k]

    def forward(c, carry):
        here = pl.ds(pl.multiple_of(c * chunk, chunk), chunk)
        sent = nn(extended[...], selector[c, :width, :]).astype(BF)
        linear = nn(edge_first_t[:, :features], sent) + slope[:, here]
        logistic = jax.nn.sigmoid(linear)
        lively = (linear * logistic).astype(BF)
        slope[:, here] = logistic * (1.0 + linear * (1.0 - logistic))
        active[:, here] = lively
        scaled, spread = standardize(nn(edge_second_t, lively))
        scaled_all[:, here] = scaled
        spread_all[:, here] = spread
        message = (scaled * edge_gain + edge_shift).astype(BF)
        summed[...] += nt(selector[c, width:, :], message)
        return carry

    lax.fori_loop(0, faces // chunk, forward, 0)

    node_first_t = node_first_ref[...]
    node_first = flip(node_first_t).astype(BF)
    node_second_t = flip(node_second_ref[...]).astype(BF)
    node_input = jnp.concatenate([node_ref[...], summed[...].T.astype(BF)], axis=0)
    node_linear = nn(node_first_t, node_input) + node_bias
    node_logistic = jax.nn.sigmoid(node_linear)
    node_active = (node_linear * node_logistic).astype(BF)
    node_scaled, node_spread = standardize(nn(node_second_t, node_active))
    upstream = node_cot_ref[...].astype(F32)
    lanes[3] = fold_lanes(upstream * node_scaled)
    lanes[4] = fold_lanes(upstream)
    node_delta = normalize_back(upstream, node_scaled, node_spread, node_gain).astype(BF)
    node_slope = node_logistic * (1.0 + node_linear * (1.0 - node_logistic))
    node_hidden = nn(node_second_ref[...], node_delta) * node_slope
    lanes[5] = fold_lanes(node_hidden)
    node_hidden = node_hidden.astype(BF)
    node_first_delta = nt(node_input, node_hidden)
    half, mid, top = packed_rows(features)
    packed_ref[half:mid, :features] = node_first_delta[:features]
    packed_ref[half:mid, features:] = node_first_delta[features:]
    packed_ref[mid:top, features:] = nt(node_active, node_delta)
    node_back = nn(node_first, node_hidden)
    local[...] = node_back[:features] + upstream
    toward = node_back[features:]
    high = toward.astype(BF)
    low = (toward - high.astype(F32)).astype(BF)
    toward = jnp.concatenate([high, low], axis=0)

    small[...] = jnp.zeros(small.shape, F32)
    for i in range(3):
        lanes[i] = jnp.zeros(lanes.shape[1:], F32)

    def backward(c, carry):
        here = pl.ds(pl.multiple_of(c * chunk, chunk), chunk)
        gathered = nn(toward, selector[c, width:, :])
        cotangent = edge_cot_ref[:, here].astype(F32)
        delta = cotangent + (gathered[:features] + gathered[features:])
        scaled = scaled_all[:, here]
        lanes[0] += fold_lanes(delta * scaled)
        lanes[1] += fold_lanes(delta)
        edge_delta = normalize_back(delta, scaled, spread_all[:, here], edge_gain).astype(BF)
        small[0] += nt(active[:, here], edge_delta)
        hidden = nn(edge_second, edge_delta) * slope[:, here]
        lanes[2] += fold_lanes(hidden)
        hidden = hidden.astype(BF)
        active[:, here] = hidden
        small[1] += nt(edge_ref[:, here], hidden)
        return carry

    lax.fori_loop(0, faces // chunk, backward, 0)
    block = math.gcd(width + cells, 512)

    def gather_sums(i, carry):
        at = pl.ds(pl.multiple_of(i * block, block), block)
        total = nt(selector[0, at, :], active[:, :chunk])
        for c in range(1, faces // chunk):
            total = total + nt(selector[c, at, :], active[:, c * chunk : (c + 1) * chunk])
        sums[at, :] = total
        return carry

    lax.fori_loop(0, (width + cells) // block, gather_sums, 0)

    by_sender = sums[:width, :].astype(BF)
    by_receiver = sums[width:, :].astype(BF)
    back = nt(edge_first[:features], by_sender)
    for k in range(peers):
        returning[k] = back[:, cells + k * halo : cells + (k + 1) * halo].astype(BF)
    first = nn(extended[...], by_sender)
    second = nn(node_ref[...], by_receiver)
    packed_ref[0:features, :features] = first
    packed_ref[features:half, :features] = second[: half - features]
    packed_ref[0 : 2 * features - half, features:] = second[half - features :]
    packed_ref[2 * features - half : half, features:] = small[1]
    packed_ref[mid:top, :features] = small[0]
    column = lax.broadcasted_iota(jnp.int32, (features, 128), 1)
    vectors = jnp.zeros((features, 128), F32)
    for i in range(6):
        vectors = jnp.where(column == i, jnp.sum(lanes[i], axis=1, keepdims=True), vectors)
    packed_ref[top:, :] = jnp.zeros((packed_ref.shape[0] - top, 128), F32)
    packed_ref[top : top + 8, :features] = vectors.T[:8]

    def part_copy(source, landing, device):
        return pltpu.make_async_remote_copy(
            src_ref=packed_ref.at[pl.ds(pl.multiple_of(source * rows, 8), rows)],
            dst_ref=pieces.at[landing],
            send_sem=part_send.at[source],
            recv_sem=part_recv.at[landing],
            device_id=device,
            device_id_type=MESH,
        )

    def whole_copy(landing, device, other):
        return pltpu.make_async_remote_copy(
            src_ref=reduced,
            dst_ref=sum_ref.at[pl.ds(pl.multiple_of(landing * rows, 8), rows)],
            send_sem=whole_send.at[other],
            recv_sem=whole_recv.at[landing],
            device_id=device,
            device_id_type=MESH,
        )

    def send_part(r, carry):
        other, device = place(r)
        part_copy(other, me, device).start()
        return carry

    lax.fori_loop(1, count, send_part, 0)
    start_exchange(dom, sub, s, returning, returned, back_send, back_recv, forward=False)
    local[...] += back[:, :cells] + nt(edge_first[features : 2 * features], by_receiver)

    def emit(c, carry):
        here = pl.ds(pl.multiple_of(c * chunk, chunk), chunk)
        ahead = nn(edge_first[2 * features :], active[:, here])
        edge_out_ref[:, here] = (edge_cot_ref[:, here].astype(F32) + ahead).astype(BF)
        return carry

    lax.fori_loop(0, faces // chunk, emit, 0)
    own = pl.ds(pl.multiple_of(me * rows, 8), rows)

    def take_part(r, total):
        other, device = place(r)
        part_copy(other, other, device).wait_recv()
        return total + pieces[other]

    reduced[...] = lax.fori_loop(1, count, take_part, packed_ref[own, :])

    def send_whole(r, carry):
        other, device = place(r)
        whole_copy(me, device, other).start()
        return carry

    lax.fori_loop(1, count, send_whole, 0)
    sum_ref[own, :] = reduced[...]
    finish_exchange(dom, sub, s, returning, returned, back_send, back_recv, forward=False)
    summed[...] = jnp.zeros(summed.shape, F32)

    def scatter(i, carry):
        value = jnp.concatenate([returned[2 * i], returned[2 * i + 1]], axis=1)
        summed[...] += nt(exports[i], value)
        return carry

    lax.fori_loop(0, peers // 2, scatter, 0)
    state_ref[...] = (local[...] + summed[...].T).astype(BF)

    def settle(r, carry):
        other, device = place(r)
        part_copy(other, other, device).wait_send()
        whole_copy(other, device, other).wait_send()
        whole_copy(other, device, other).wait_recv()
        return carry

    lax.fori_loop(1, count, settle, 0)


def unpack_kernel(
    factor, state_in, edge_in, sum_ref,
    state_ref, edge_ref, edge_first_ref, edge_second_ref, node_first_ref, node_second_ref, *vector_refs,
):
    features = state_in.shape[0]
    half, mid, top = packed_rows(features)
    state_ref[...] = state_in[...]
    edge_ref[...] = edge_in[...]
    left = sum_ref[:, :features] * factor
    right = sum_ref[:, features:] * factor
    edge_first_ref[...] = jnp.concatenate([left[:half], right[:half]], axis=0).T
    node_first_ref[...] = jnp.concatenate([left[half:mid], right[half:mid]], axis=0).T
    edge_second_ref[...] = left[mid:top]
    node_second_ref[...] = right[mid:top]
    for i, vector_ref in enumerate(vector_refs):
        vector_ref[...] = left[top + i : top + i + 1]


def on_device(
    dom, sub,
    node_state, edge_state, senders, receivers, send_index, node_cotangent, edge_cotangent,
    edge_first, edge_bias, edge_second, edge_gain, edge_shift, node_first, node_bias, node_second, node_gain,
):
    features, cells = node_state.shape
    faces = edge_state.shape[1]
    halo = send_index.shape[2]
    peers = 3 * sub
    ghosts = peers * halo
    width = cells + ghosts
    count = dom * sub
    rows = -(-(packed_rows(features)[2] + 8) // (8 * count)) * 8
    chunk = math.gcd(faces, 512)
    vmem = pl.BlockSpec(memory_space=pltpu.VMEM)
    shape = jax.ShapeDtypeStruct
    dma = pltpu.SemaphoreType.DMA

    def line(vector):
        return vector.reshape(1, -1)

    state, edge_result, total = pl.pallas_call(
        functools.partial(layer_kernel, dom, sub, chunk),
        out_shape=(
            shape((features, cells), BF),
            shape((features, faces), BF),
            shape((count * rows, 128), F32),
        ),
        in_specs=[vmem] * 16,
        out_specs=(vmem,) * 3,
        scratch_shapes=[pltpu.VMEM((peers, features, halo), BF)] * 4
        + [
            pltpu.VMEM((peers // 2, cells, 2 * halo), BF),
            pltpu.VMEM((faces // chunk, width + cells, chunk), BF),
            pltpu.VMEM((features, width), BF),
            pltpu.VMEM((features, faces), F32),
            pltpu.VMEM((features, faces), BF),
            pltpu.VMEM((features, faces), F32),
            pltpu.VMEM((1, faces), F32),
            pltpu.VMEM((cells, features), F32),
            pltpu.VMEM((width + cells, features), F32),
            pltpu.VMEM((2, features, features), F32),
            pltpu.VMEM((6, features, 128), F32),
            pltpu.VMEM((features, cells), F32),
            pltpu.VMEM((count * rows, 128), F32),
            pltpu.VMEM((count, rows, 128), F32),
            pltpu.VMEM((rows, 128), F32),
        ]
        + [dma((peers,))] * 4
        + [dma((count,))] * 4,
        compiler_params=pltpu.CompilerParams(
            collective_id=0, has_side_effects=True, vmem_limit_bytes=60 * 1024 * 1024
        ),
        name="layer",
    )(
        node_state, edge_state, line(senders), line(receivers), line(send_index),
        node_cotangent, edge_cotangent, edge_first.T, edge_second, node_first.T, node_second,
        line(edge_bias), line(edge_gain), line(edge_shift), line(node_bias), line(node_gain),
    )
    vector = shape((1, features), F32)
    state, edge_result, edge_first_sum, edge_second_sum, node_first_sum, node_second_sum, *vectors = pl.pallas_call(
        functools.partial(unpack_kernel, 1.0 / math.sqrt(faces * count)),
        out_shape=(
            shape((features, cells), BF),
            shape((features, faces), BF),
            shape(edge_first.shape[::-1], F32),
            shape(edge_second.shape, F32),
            shape(node_first.shape[::-1], F32),
            shape(node_second.shape, F32),
        )
        + (vector,) * 6,
        in_specs=[vmem] * 3,
        out_specs=(vmem,) * 12,
        name="unpack",
    )(state, edge_result, total)
    vectors = [v.reshape(-1) for v in vectors]
    return (
        state, edge_result, edge_first_sum.T, vectors[2], edge_second_sum, vectors[0], vectors[1],
        node_first_sum.T, vectors[5], node_second_sum, vectors[3], vectors[4],
    )


def solution(mesh):
    split = P(None, ("dom", "sub"))
    faces = P(("dom", "sub"))
    return jax.shard_map(
        functools.partial(on_device, mesh.shape["dom"], mesh.shape["sub"]),
        mesh=mesh,
        in_specs=(split, split, faces, faces, P(("dom", "sub"), None, None), split, split) + (P(),) * 9,
        out_specs=(split, split) + (P(),) * 10,
        check_vma=False,
    )
```
